32 devices in a mesh: dp: 4 (over y, z), tp: 8 (over x, core).
Axes of the slice: x: 4, y: 2, z: 2, core: 2. Of those that a mesh axis runs over, the one named last changes fastest.
The devices are a block of a 4x4x8 slice.
Arguments:
- x: bfloat16 [4, 2048, 4096], P('dp', 'tp'), parts along dimension 0
- ln_gain: bfloat16 [2, 4096], replicated
- ln_bias: bfloat16 [2, 4096], replicated
- w_q: bfloat16 [2, 4096, 16, 256], P(None, None, 'tp')
- b_q: bfloat16 [2, 16, 256], P(None, 'tp')
- w_k: bfloat16 [2, 4096, 16, 256], P(None, None, 'tp')
- b_k: bfloat16 [2, 16, 256], P(None, 'tp')
- w_v: bfloat16 [2, 4096, 16, 256], P(None, None, 'tp')
- b_v: bfloat16 [2, 16, 256], P(None, 'tp')
- w_o: bfloat16 [2, 16, 256, 4096], P(None, 'tp')
- b_o: bfloat16 [2, 4096], replicated
- w_up: bfloat16 [2, 4096, 16384], P(None, None, 'tp')
- b_up: bfloat16 [2, 16384], P(None, 'tp')
- w_down: bfloat16 [2, 16384, 4096], P(None, 'tp')
- b_down: bfloat16 [2, 4096], replicated
Outputs:
- output: bfloat16 [4, 2048, 4096], P('dp', 'tp'), parts along dimension 0
There are 4 independent parts. The reference program is written for one: setup_inputs(seed, part) draws one part's arguments, and reference() takes and returns one part's arrays. A program takes and returns all parts, laid end to end along the dimension named above; an argument that names none is the same for every part.
All inputs are finite; a program needn't handle non-finite values.
Results may differ from the reference program's by a relative error of at most 0.0171331.
Values are sent between devices in bfloat16 or wider.
A program may use at most 768 MiB of HBM per device.

```python
import jax
import jax.numpy as jnp
from jax import lax

N_BATCH = 1
SEQ_LEN = 2048
D_MODEL = 4096
N_HEADS = 16
HEAD_DIM = 256
D_FF = 16384
ROT_DIM = 32
N_LAYERS = 2


def setup_inputs(seed: int = 0, part: int = 0) -> dict:
    shared_keys = jax.random.split(jax.random.key(seed), 14)
    token_key = jax.random.fold_in(jax.random.key(seed + 1), part)

    def draw(key_index, shape, scale, offset):
        sample = jax.random.normal(shared_keys[key_index], shape, jnp.float32)
        return (offset + scale * sample).astype(jnp.bfloat16)

    proj_shape = (N_LAYERS, D_MODEL, N_HEADS, HEAD_DIM)
    head_shape = (N_LAYERS, N_HEADS, HEAD_DIM)
    wide_shape = (N_LAYERS, D_MODEL)
    in_scale = D_MODEL ** -0.5
    x = jax.random.normal(token_key, (N_BATCH, SEQ_LEN, D_MODEL), jnp.float32).astype(jnp.bfloat16)
    return {
        "x": x,
        "ln_gain": draw(0, wide_shape, 0.3, 1.0),
        "ln_bias": draw(1, wide_shape, 0.3, 0.0),
        "w_q": draw(2, proj_shape, 2.0 * in_scale, 0.0),
        "b_q": draw(3, head_shape, 0.5, 0.0),
        "w_k": draw(4, proj_shape, 2.0 * in_scale, 0.0),
        "b_k": draw(5, head_shape, 0.5, 0.0),
        "w_v": draw(6, proj_shape, in_scale, 0.0),
        "b_v": draw(7, head_shape, 0.5, 0.0),
        "w_o": draw(8, (N_LAYERS, N_HEADS, HEAD_DIM, D_MODEL), in_scale, 0.0),
        "b_o": draw(9, wide_shape, 0.5, 0.0),
        "w_up": draw(10, (N_LAYERS, D_MODEL, D_FF), in_scale, 0.0),
        "b_up": draw(11, (N_LAYERS, D_FF), 0.5, 0.0),
        "w_down": draw(12, (N_LAYERS, D_FF, D_MODEL), D_FF ** -0.5, 0.0),
        "b_down": draw(13, wide_shape, 0.5, 0.0),
    }


def rotary_tables():
    half = ROT_DIM // 2
    inv_freq = 1.0 / (10000.0 ** (jnp.arange(half, dtype=jnp.float32) * (2.0 / ROT_DIM)))
    angles = jnp.arange(SEQ_LEN, dtype=jnp.float32)[:, None] * inv_freq[None, :]
    return jnp.cos(angles)[:, None, :], jnp.sin(angles)[:, None, :]


def apply_rotary(projected, cosine, sine):
    half = ROT_DIM // 2
    first = projected[..., :half]
    second = projected[..., half:ROT_DIM]
    return jnp.concatenate([first * cosine - second * sine, second * cosine + first * sine, projected[..., ROT_DIM:]], axis=-1)


def attend_heads(q_rot, k_rot, values):
    def per_head(operands):
        q_one, k_one, v_one = operands
        scores = jnp.dot(q_one, jnp.transpose(k_one), preferred_element_type=jnp.float32) * (HEAD_DIM ** -0.5)
        causal = jnp.arange(SEQ_LEN)[:, None] >= jnp.arange(SEQ_LEN)[None, :]
        attn_probs = jax.nn.softmax(jnp.where(causal, scores, -1e30), axis=-1).astype(jnp.bfloat16)
        return jnp.dot(attn_probs, v_one, preferred_element_type=jnp.float32).astype(jnp.bfloat16)

    def by_head(tensor):
        return jnp.transpose(tensor, (0, 2, 1, 3)).reshape(N_BATCH * N_HEADS, SEQ_LEN, HEAD_DIM)

    head_out = lax.map(per_head, (by_head(q_rot), by_head(k_rot), by_head(values)))
    return jnp.transpose(head_out.reshape(N_BATCH, N_HEADS, SEQ_LEN, HEAD_DIM), (0, 2, 1, 3))


def layer_forward(hidden, layer_params):
    (ln_gain, ln_bias, w_q, b_q, w_k, b_k, w_v, b_v, w_o, b_o, w_up, b_up, w_down, b_down) = layer_params
    x_f32 = hidden.astype(jnp.float32)
    mean = jnp.mean(x_f32, axis=-1, keepdims=True)
    centered = x_f32 - mean
    variance = jnp.mean(centered * centered, axis=-1, keepdims=True)
    normed = (centered * lax.rsqrt(variance + 1e-5) * ln_gain.astype(jnp.float32) + ln_bias.astype(jnp.float32)).astype(jnp.bfloat16)
    flat = normed.reshape(N_BATCH * SEQ_LEN, D_MODEL)
    head_shape = (N_BATCH, SEQ_LEN, N_HEADS, HEAD_DIM)
    cosine, sine = rotary_tables()

    def project(weight, bias):
        prod = jnp.dot(flat, weight.reshape(D_MODEL, N_HEADS * HEAD_DIM), preferred_element_type=jnp.float32)
        return prod.reshape(head_shape) + bias.astype(jnp.float32)

    q_rot = apply_rotary(project(w_q, b_q), cosine, sine).astype(jnp.bfloat16)
    k_rot = apply_rotary(project(w_k, b_k), cosine, sine).astype(jnp.bfloat16)
    values = project(w_v, b_v).astype(jnp.bfloat16)
    attended = attend_heads(q_rot, k_rot, values)
    dense_out = jnp.dot(attended.reshape(N_BATCH * SEQ_LEN, D_MODEL), w_o.reshape(D_MODEL, D_MODEL), preferred_element_type=jnp.float32)
    up_act = jax.nn.gelu(jnp.dot(flat, w_up, preferred_element_type=jnp.float32) + b_up.astype(jnp.float32), approximate=True).astype(jnp.bfloat16)
    down_out = jnp.dot(up_act, w_down, preferred_element_type=jnp.float32)
    total = x_f32.reshape(N_BATCH * SEQ_LEN, D_MODEL) + dense_out + down_out + b_o.astype(jnp.float32) + b_down.astype(jnp.float32)
    return total.reshape(N_BATCH, SEQ_LEN, D_MODEL).astype(jnp.bfloat16)


def reference(x, ln_gain, ln_bias, w_q, b_q, w_k, b_k, w_v, b_v, w_o, b_o, w_up, b_up, w_down, b_down):
    stacked = (ln_gain, ln_bias, w_q, b_q, w_k, b_k, w_v, b_v, w_o, b_o, w_up, b_up, w_down, b_down)

    def layer_body(hidden, layer_params):
        return layer_forward(hidden, layer_params), None

    final = lax.scan(layer_body, x, stacked)
    return final[0]
```

```python
import functools

import jax
import jax.numpy as jnp
import numpy as np
from jax import lax
from jax.experimental import pallas as pl
from jax.experimental.pallas import tpu as pltpu
from jax.sharding import PartitionSpec as P

BF16, F32 = jnp.bfloat16, jnp.float32
MESH = pl.DeviceIdType.MESH
ROT_DIM, ROPE_BASE, LN_EPS = 32, 10000.0, 1e-5
CHIPS, GROUPS, R = 4, 4, 64
SUB = 2 * R
CHUNK = GROUPS * SUB
VMEM_LIMIT = 66_900_000


def rotary_constants(seq_len):
    inv_freq = 1.0 / ROPE_BASE ** (np.arange(ROT_DIM // 2) * (2.0 / ROT_DIM))

    def table(positions):
        angles = positions[:, None] * inv_freq[None, :]
        cos, sin = np.ones((len(positions), 128)), np.zeros((len(positions), 128))
        cos[:, :ROT_DIM] = np.concatenate([np.cos(angles), np.cos(angles)], axis=1)
        sin[:, :ROT_DIM] = np.concatenate([-np.sin(angles), np.sin(angles)], axis=1)
        return cos.astype(np.float32), sin.astype(np.float32)

    return table(np.arange(R, dtype=np.float64)) + table(np.arange(0, seq_len, R, dtype=np.float64))


def place():
    tp = lax.axis_index("tp")
    chip, core = tp // 2, tp % 2
    right = {"tp": ((chip + 1) % CHIPS) * 2 + core}
    left = {"tp": ((chip + CHIPS - 1) % CHIPS) * 2 + core}
    sibling = {"tp": chip * 2 + 1 - core}
    return chip, core, right, left, sibling


def greet(peers):
    barrier = pltpu.get_barrier_semaphore()
    for peer in peers:
        pl.semaphore_signal(barrier, inc=1, device_id=peer, device_id_type=MESH)
    pl.semaphore_wait(barrier, len(peers))


def rows_at(start, size):
    return pl.ds(pl.multiple_of(start, R), size)


def remote(src, dst, send, recv, peer):
    return pltpu.make_async_remote_copy(src_ref=src, dst_ref=dst, send_sem=send, recv_sem=recv, device_id=peer, device_id_type=MESH)


def gelu(x):
    inner = x * (0.7978845608028654 + (0.7978845608028654 * 0.044715) * (x * x))
    return x * (0.5 + 0.5 * jnp.tanh(inner))


def project_kernel(layer, x_ref, gain_ref, bias_ref, bq_ref, bk_ref, bv_ref, bup_ref, cosr_ref, sinr_ref, cosb_ref, sinb_ref,
                   wq_hbm, wk_hbm, wv_hbm, wup_hbm, y_hbm, h_buf, wqkv, wup, raw, out_buf,
                   near_send, near_recv, far_send, far_recv, sib_send, sib_recv, up_sem, raw_sem, out_sem):
    chip, core, right, left, sibling = place()
    depth, width = wup.shape
    head = wq_hbm.shape[3]
    qkv = 2 * head
    n_up = width // 512
    kstep = raw.shape[1]
    slots = raw.shape[0]
    per = depth // kstep
    total_raw = 3 * per

    def up_copy(n):
        cols = pl.ds(n * 512, 512)
        return pltpu.make_async_copy(wup_hbm.at[layer, :, cols], wup.at[:, cols], up_sem.at[n])

    def raw_copy(j):
        w = (wq_hbm, wk_hbm, wv_hbm)[j // per]
        return pltpu.make_async_copy(w.at[layer, pl.ds((j % per) * kstep, kstep)], raw.at[j % slots], raw_sem.at[j % slots])

    for j in range(slots):
        raw_copy(j).start()
    for n in range(n_up):
        up_copy(n).start()
    greet((right, left, sibling))

    def group(c, g, k):
        return h_buf.at[rows_at(c * CHUNK + g * SUB + k * R, R)]

    left_chip, right_chip, far_chip = (chip + CHIPS - 1) % CHIPS, (chip + 1) % CHIPS, (chip + 2) % CHIPS

    def near(side, g):
        blk = group(chip, g, core)
        return remote(blk, blk, near_send.at[side, g], near_recv.at[side, g], (right, left)[side])

    def near_in(side, g):
        blk = group((left_chip, right_chip)[side], g, core)
        return remote(blk, blk, near_send.at[side, g], near_recv.at[side, g], (right, left)[side])

    def far(side, b):
        blk = group((left_chip, right_chip)[side], side * 2 + b, core)
        return remote(blk, blk, far_send.at[side, b], far_recv.at[side, b], (right, left)[side])

    def far_in(side, b):
        blk = group(far_chip, side * 2 + b, core)
        return remote(blk, blk, far_send.at[side, b], far_recv.at[side, b], (right, left)[side])

    def share(slot, c, g, k):
        blk = group(c, g, k)
        return remote(blk, blk, sib_send.at[slot, g], sib_recv.at[slot, g], sibling)

    gain = gain_ref[layer:layer + 1, :].astype(F32)
    bias = bias_ref[layer:layer + 1, :].astype(F32)

    def normalize(g):
        def strip(j, carry):
            x = x_ref[pl.ds(pl.multiple_of(g * R + j * 16, 16), 16), :].astype(F32)
            mean = jnp.mean(x, axis=-1, keepdims=True)
            cen = x - mean
            var = jnp.mean(cen * cen, axis=-1, keepdims=True)
            out = (cen * lax.rsqrt(var + LN_EPS) * gain + bias).astype(BF16)
            h_buf[pl.ds(pl.multiple_of(chip * CHUNK + g * SUB + core * R + j * 16, 16), 16), :] = out
            return carry
        lax.fori_loop(0, R // 16, strip, 0)

    for g, side in ((0, 0), (2, 1), (1, 0), (3, 1)):
        normalize(g)
        near(side, g).start()
        share(0, chip, g, core).start()
    for g, side in ((2, 0), (0, 1), (3, 0), (1, 1)):
        near(side, g).start()

    for j in range(total_raw):
        raw_copy(j).wait()
        x = jnp.swapaxes(raw[j % slots], 0, 1)
        for hd in range(2):
            wqkv[pl.ds((j % per) * kstep, kstep), pl.ds((j // per) * qkv + hd * head, head)] = x[hd]
        if j + slots < total_raw:
            raw_copy(j + slots).start()
    for n in range(n_up):
        up_copy(n).wait()

    def exchange(b):
        for side in range(2):
            g = (b + 2 * side) % GROUPS
            near_in(side, g).wait_recv()
            share(1 + side, (left_chip, right_chip)[side], g, core).start()

            @pl.when(b < 2)
            def _():
                far(side, b).start()

    def exchange_far(b):
        for side in range(2):
            far_in(side, b).wait_recv()
            share(3, far_chip, side * 2 + b, core).start()

    lane = lax.broadcasted_iota(jnp.int32, (SUB, 128), 1)

    def out_copy(slot, row0):
        return pltpu.make_async_copy(out_buf.at[slot], y_hbm.at[rows_at(row0, SUB)], out_sem.at[slot])

    def coords(i):
        near_b, near_s = (i - 4) // 2, (i - 4) % 2
        far_b, far_s = (i - 12) // 2, (i - 12) % 2
        is_own, is_far = i < 4, i >= 12
        slot = jnp.where(is_own, 0, jnp.where(is_far, 3, 1 + near_s))
        c = (chip + jnp.where(is_own, 0, jnp.where(is_far, 2, jnp.where(near_s == 0, CHIPS - 1, 1)))) % CHIPS
        g = jnp.where(is_own, i, jnp.where(is_far, far_s * 2 + far_b, (near_b + 2 * near_s) % GROUPS))
        return slot, c, g

    def piece(i, carry):
        @pl.when(jnp.logical_and(jnp.logical_and(i >= 3, i <= 9), i % 2 == 1))
        def _():
            exchange((i - 3) // 2)

        @pl.when(i == 11)
        def _():
            exchange_far(0)

        @pl.when(i == 14)
        def _():
            exchange_far(1)

        slot, c, g = coords(i)
        share(slot, c, g, 1 - core).wait_recv()
        row0 = c * CHUNK + g * SUB
        rows = rows_at(row0, SUB)
        o = i % 2

        @pl.when(i >= 2)
        def _():
            _, c2, g2 = coords(i - 2)
            out_copy(o, c2 * CHUNK + g2 * SUB).wait()

        for n in range(n_up):
            cols = slice(n * 512, (n + 1) * 512)
            acc = jnp.dot(h_buf[rows, :], wup[:, cols], preferred_element_type=F32) + bup_ref[layer:layer + 1, cols].astype(F32)
            out_buf[o, :, 3 * qkv + n * 512:3 * qkv + (n + 1) * 512] = gelu(acc).astype(BF16)
        pos_blk = c * (CHUNK // R) + g
        for j, b_ref in enumerate((bq_ref, bk_ref, bv_ref)):
            acc = jnp.dot(h_buf[rows, :], wqkv[:, j * qkv:(j + 1) * qkv], preferred_element_type=F32)
            for hd in range(2):
                lo = j * qkv + hd * head
                val = acc[:, hd * head:(hd + 1) * head] + b_ref[layer, hd:hd + 1, :].astype(F32)
                if j == 2:
                    out_buf[o, :, lo:lo + head] = val.astype(BF16)
                    continue
                u = val[:, :128]
                partner = jnp.where(lane < ROT_DIM // 2, pltpu.roll(u, 128 - ROT_DIM // 2, 1), pltpu.roll(u, ROT_DIM // 2, 1))
                for k in range(2):
                    cb = cosb_ref[pl.ds(pos_blk + k * GROUPS, 1), :]
                    sb = sinb_ref[pl.ds(pos_blk + k * GROUPS, 1), :]
                    cos = cb * cosr_ref[...] - sb * sinr_ref[...]
                    sin = sb * cosr_ref[...] + cb * sinr_ref[...]
                    part = slice(k * R, (k + 1) * R)
                    out_buf[o, part, lo:lo + 128] = (u[part] * cos + partner[part] * sin).astype(BF16)
                out_buf[o, :, lo + 128:lo + head] = val[:, 128:].astype(BF16)
        out_copy(o, row0).start()
        return carry

    lax.fori_loop(0, 16, piece, 0)
    for i in (14, 15):
        _, c, g = coords(i)
        out_copy(i % 2, c * CHUNK + g * SUB).wait()
    for g in range(GROUPS):
        for side in range(2):
            near(side, g).wait_send()
        for slot in range(4):
            share(slot, (chip, left_chip, right_chip, far_chip)[slot], g, core).wait_send()
    for side in range(2):
        for b in range(2):
            far(side, b).wait_send()


def project(layer, x, ln_gain, ln_bias, w_q, b_q, w_k, b_k, w_v, b_v, w_up, b_up, tables):
    depth, width = w_up.shape[1:]
    seq = CHIPS * CHUNK
    qkv = 3 * w_q.shape[2] * w_q.shape[3]
    vmem, hbm = pl.BlockSpec(memory_space=pltpu.VMEM), pl.BlockSpec(memory_space=pltpu.HBM)
    dma = pltpu.SemaphoreType.DMA
    flops = 2 * seq * depth * (qkv + width)
    return pl.pallas_call(
        functools.partial(project_kernel, layer),
        out_shape=jax.ShapeDtypeStruct((seq, qkv + width), BF16),
        in_specs=[vmem] * 11 + [hbm] * 4,
        out_specs=hbm,
        scratch_shapes=[
            pltpu.VMEM((seq, depth), BF16), pltpu.VMEM((depth, qkv), BF16), pltpu.VMEM((depth, width), BF16),
            pltpu.VMEM((6, 512) + w_q.shape[2:], BF16), pltpu.VMEM((2, SUB, qkv + width), BF16),
            dma((2, 4)), dma((2, 4)), dma((2, 2)), dma((2, 2)), dma((4, 4)), dma((4, 4)), dma((width // 512,)), dma((6,)), dma((2,)),
        ],
        compiler_params=pltpu.CompilerParams(collective_id=2 * layer, has_side_effects=True, vmem_limit_bytes=VMEM_LIMIT),
        cost_estimate=pl.CostEstimate(flops=flops, bytes_accessed=60_000_000, transcendentals=seq * width),
        name=f"project_{layer}",
    )(x, ln_gain, ln_bias, b_q, b_k, b_v, b_up, *tables, w_q, w_k, w_v, w_up)


def combine_kernel(layer, x_ref, bo_ref, bd_ref, y_hbm, wo_hbm, wd_hbm, out_ref,
                   wo, wd, keys, vals, q_buf, a_buf, s_buf, o_buf, att, part, sib_in, far_in, fin_in, send_buf,
                   w_sem, q_sem, a_sem, sib_send, sib_recv, ici_send, far_recv, fin_recv):
    chip, core, right, left, sibling = place()
    qkv = wo.shape[0]
    head = qkv // 2
    inner, depth = wd.shape
    left_chip, right_chip, far_chip = (chip + CHIPS - 1) % CHIPS, (chip + 1) % CHIPS, (chip + 2) % CHIPS

    def where_is(i):
        s, b = i % 2, (i // 2) % 2
        stage = i // 4
        c = jnp.where(stage == 0, far_chip, jnp.where(stage == 3, chip, jnp.where(s == 0, right_chip, left_chip)))
        half = jnp.where(stage == 1, 1 - s, s)
        return c, half * 2 + b

    def row_of(i):
        c, g = where_is(i)
        return c * CHUNK + g * SUB

    def q_copy(i):
        return pltpu.make_async_copy(y_hbm.at[rows_at(row_of(i), SUB), pl.ds(0, qkv)], q_buf.at[i], q_sem.at[i])

    def a_copy(i):
        return pltpu.make_async_copy(y_hbm.at[rows_at(row_of(i), SUB), pl.ds(3 * qkv, inner)], a_buf.at[i], a_sem.at[i])

    loads = [pltpu.make_async_copy(y_hbm.at[:, pl.ds(qkv, qkv)], keys, w_sem.at[0]),
             pltpu.make_async_copy(y_hbm.at[:, pl.ds(2 * qkv, qkv)], vals, w_sem.at[1]),
             pltpu.make_async_copy(wo_hbm.at[layer], wo, w_sem.at[2])]
    wd_loads = [pltpu.make_async_copy(wd_hbm.at[layer, :, pl.ds(n * 1024, 1024)], wd.at[:, pl.ds(n * 1024, 1024)], w_sem.at[3 + n])
                for n in range(depth // 1024)]
    q_copy(0).start()
    a_copy(0).start()
    for cp in loads + wd_loads:
        cp.start()
    for i in range(1, 16):
        q_copy(i).start()
        a_copy(i).start()
    greet((right, left, sibling))

    scale = (head ** -0.5) * 1.4426950408889634
    krow = lax.broadcasted_iota(jnp.int32, (SUB, CHUNK), 1)
    kpos = (krow // R % 2) * (CHUNK // 2) + (krow // SUB) * R + krow % R
    qrow = lax.broadcasted_iota(jnp.int32, (SUB, CHUNK), 0)

    def lanes(x, op):
        r = x[:, 0:128]
        for j in range(1, x.shape[1] // 128):
            r = op(r, x[:, j * 128:(j + 1) * 128])
        return r

    def attend(i):
        t, g = where_is(i)
        qpos = (qrow // R) * (CHUNK // 2) + g * R + qrow % R

        def scores(kb, hd):
            return lax.dot_general(q_buf[i, :, hd * head:(hd + 1) * head], keys[rows_at(kb * CHUNK, CHUNK), hd * head:(hd + 1) * head],
                                   (((1,), (1,)), ((), ())), preferred_element_type=F32)

        top = []
        for hd in range(2):
            s = jnp.where(qpos >= kpos, scores(t, hd), -1e30)
            s_buf[hd, t] = s
            top.append(lanes(s, jnp.maximum))

        def first(kb, top):
            new = []
            for hd in range(2):
                s = scores(kb, hd)
                s_buf[hd, kb] = s
                new.append(jnp.maximum(top[hd], lanes(s, jnp.maximum)))
            return tuple(new)

        top = lax.fori_loop(0, t, first, tuple(top))
        top = [jnp.max(m, axis=1, keepdims=True) * scale for m in top]

        def second(kb, tot):
            new = []
            for hd in range(2):
                e = jnp.exp2(s_buf[hd, kb] * scale - top[hd])
                s_buf[hd, kb] = e
                new.append(tot[hd] + lanes(e, jnp.add))
            return tuple(new)

        zero = jnp.zeros((SUB, 128), F32)
        tot = lax.fori_loop(0, t + 1, second, (zero, zero))
        inv = [1.0 / jnp.sum(v, axis=1, keepdims=True) for v in tot]

        def weighted(kb, hd):
            p = (s_buf[hd, kb] * inv[hd]).astype(BF16)
            return jnp.dot(p, vals[rows_at(kb * CHUNK, CHUNK), hd * head:(hd + 1) * head], preferred_element_type=F32)

        for hd in range(2):
            o_buf[hd] = weighted(t, hd)

        def third(kb, carry):
            for hd in range(2):
                o_buf[hd] += weighted(kb, hd)
            return carry

        lax.fori_loop(0, t, third, 0)
        for hd in range(2):
            att[:, hd * head:(hd + 1) * head] = o_buf[hd].astype(BF16)

    def to_sibling(i):
        return remote(part.at[i % 2, rows_at((1 - core) * R, R)], sib_in.at[i % 4], sib_send.at[i % 2], sib_recv.at[i % 4], sibling)

    def out_far(i):
        s, b = i % 2, i // 2
        return [remote(send_buf.at[i], far_in.at[side, b], ici_send.at[i], far_recv.at[side, b], (right, left)[side]) for side in range(2)], s

    def out_fin(i):
        s = i % 2
        _, g = where_is(i)
        return [remote(send_buf.at[i], fin_in.at[side, g], ici_send.at[i], fin_recv.at[side, g], (right, left)[side]) for side in range(2)], s

    def start_by_side(pair):
        copies, s = pair
        for side in range(2):
            @pl.when(s == side)
            def _():
                copies[side].start()

    STRIP = 16

    def merge(i, extra):
        to_sibling(i).wait_recv()

        def strip(j, carry):
            r = pl.ds(pl.multiple_of(j * STRIP, STRIP), STRIP)
            v = part[i % 2, pl.ds(pl.multiple_of(core * R + j * STRIP, STRIP), STRIP), :].astype(F32) + sib_in[i % 4, r, :].astype(F32)
            if extra:
                v += far_in[i % 2, (i // 2) % 2, r, :].astype(F32)
            send_buf[i, r, :] = v.astype(BF16)
            return carry

        lax.fori_loop(0, R // STRIP, strip, 0)

    def settle(i):
        @pl.when(i < 4)
        def _():
            merge(i, False)
            start_by_side(out_far(i))

        @pl.when(jnp.logical_and(i >= 4, i < 8))
        def _():
            merge(i, False)
            start_by_side(out_fin(i))

        @pl.when(jnp.logical_and(i >= 8, i < 12))
        def _():
            s, b = i % 2, (i // 2) % 2
            for side in range(2):
                @pl.when(s == side)
                def _():
                    remote(send_buf.at[i], far_in.at[side, b], ici_send.at[i], far_recv.at[side, b], (right, left)[side]).wait_recv()
            merge(i, True)
            start_by_side(out_fin(i))

        @pl.when(i >= 12)
        def _():
            merge(i, False)

    def piece(i, carry):
        q_copy(i).wait()

        @pl.when(i == 0)
        def _():
            loads[0].wait()
            loads[1].wait()

        attend(i)
        a_copy(i).wait()

        @pl.when(i == 0)
        def _():
            loads[2].wait()
            for cp in wd_loads:
                cp.wait()

        @pl.when(i >= 2)
        def _():
            to_sibling(i - 2).wait_send()

        for n in range(depth // 512):
            cols = slice(n * 512, (n + 1) * 512)
            acc = (jnp.dot(a_buf[i], wd[:, cols], preferred_element_type=F32)
                   + jnp.dot(att[...], wo[:, cols], preferred_element_type=F32))
            part[i % 2, :, cols] = acc.astype(BF16)
        to_sibling(i).start()

        @pl.when(i >= 1)
        def _():
            settle(i - 1)

        return carry

    lax.fori_loop(0, 16, piece, 0)
    settle(15)
    for i in (14, 15):
        to_sibling(i).wait_send()

    both = bo_ref[layer:layer + 1, :].astype(F32) + bd_ref[layer:layer + 1, :].astype(F32)
    for i in range(12, 16):
        g = (i % 2) * 2 + (i // 2) % 2
        for side in range(2):
            remote(send_buf.at[i], fin_in.at[side, g], ici_send.at[0], fin_recv.at[side, g], (right, left)[side]).wait_recv()

        def strip(j, carry):
            r = pl.ds(pl.multiple_of(j * STRIP, STRIP), STRIP)
            xr = pl.ds(pl.multiple_of(g * R + j * STRIP, STRIP), STRIP)
            v = x_ref[xr, :].astype(F32) + send_buf[i, r, :].astype(F32)
            v = v + fin_in[0, g, r, :].astype(F32) + fin_in[1, g, r, :].astype(F32) + both
            out_ref[xr, :] = v.astype(BF16)
            return carry

        lax.fori_loop(0, R // STRIP, strip, 0)
    for i in range(12):
        copies = out_far(i)[0] if i < 4 else out_fin(i)[0]
        copies[i % 2].wait_send()


def combine(layer, x, y, w_o, b_o, w_down, b_down):
    qkv, depth = w_o.shape[1:]
    inner = w_down.shape[1]
    head = qkv // 2
    seq = CHIPS * CHUNK
    vmem, hbm = pl.BlockSpec(memory_space=pltpu.VMEM), pl.BlockSpec(memory_space=pltpu.HBM)
    dma = pltpu.SemaphoreType.DMA
    return pl.pallas_call(
        functools.partial(combine_kernel, layer),
        out_shape=jax.ShapeDtypeStruct(x.shape, BF16),
        in_specs=[vmem] * 3 + [hbm] * 3,
        out_specs=vmem,
        scratch_shapes=[
            pltpu.VMEM((qkv, depth), BF16), pltpu.VMEM((inner, depth), BF16), pltpu.VMEM((seq, qkv), BF16), pltpu.VMEM((seq, qkv), BF16),
            pltpu.VMEM((16, SUB, qkv), BF16), pltpu.VMEM((16, SUB, inner), BF16), pltpu.VMEM((2, CHIPS, SUB, CHUNK), F32),
            pltpu.VMEM((2, SUB, head), F32), pltpu.VMEM((SUB, qkv), BF16), pltpu.VMEM((2, SUB, depth), BF16),
            pltpu.VMEM((4, R, depth), BF16), pltpu.VMEM((2, 2, R, depth), BF16), pltpu.VMEM((2, GROUPS, R, depth), BF16),
            pltpu.VMEM((16, R, depth), BF16),
            dma((3 + depth // 1024,)), dma((16,)), dma((16,)), dma((2,)), dma((4,)), dma((12,)), dma((2, 2)), dma((2, GROUPS)),
        ],
        compiler_params=pltpu.CompilerParams(collective_id=2 * layer + 1, has_side_effects=True, vmem_limit_bytes=VMEM_LIMIT),
        cost_estimate=pl.CostEstimate(flops=2 * seq * depth * (qkv + inner), bytes_accessed=60_000_000, transcendentals=seq * seq),
        name=f"combine_{layer}",
    )(x, b_o, b_down, y, w_o, w_down)


def solution(mesh):
    head_spec = P(None, None, "tp", None)
    head_bias_spec = P(None, "tp", None)
    in_specs = (P("dp", "tp", None), P(), P(), head_spec, head_bias_spec, head_spec, head_bias_spec, head_spec, head_bias_spec,
                P(None, "tp", None, None), P(), P(None, None, "tp"), P(None, "tp"), P(None, "tp", None), P())

    def local_program(x_loc, ln_gain, ln_bias, w_q, b_q, w_k, b_k, w_v, b_v, w_o, b_o, w_up, b_up, w_down, b_down):
        tables = [jnp.asarray(t) for t in rotary_constants(x_loc.shape[1] * mesh.shape["tp"])]
        w_o = w_o.reshape(w_o.shape[0], -1, w_o.shape[3])
        hidden = x_loc.reshape(x_loc.shape[1:])
        for layer in range(w_q.shape[0]):
            y = project(layer, hidden, ln_gain, ln_bias, w_q, b_q, w_k, b_k, w_v, b_v, w_up, b_up, tables)
            hidden = combine(layer, hidden, y, w_o, b_o, w_down, b_down)
        return hidden.reshape(x_loc.shape)

    return jax.shard_map(local_program, mesh=mesh, in_specs=in_specs, out_specs=P("dp", "tp", None), check_vma=False)
```
